32 devices in a mesh: scene: 2 (over y), cam: 16 (over z, x, core).
Axes of the slice: x: 2, y: 2, z: 4, core: 2. Of those that a mesh axis runs over, the one named last changes fastest.
Arguments:
- queries: bfloat16 [32, 768, 1024], P(('scene', 'cam')), parts along dimension 0, may hold values from -32 to 32
- keys: bfloat16 [32, 768, 1024], P(('scene', 'cam')), parts along dimension 0, may hold values from -32 to 32
- values: bfloat16 [32, 768, 1024], P(('scene', 'cam')), parts along dimension 0, may hold values from -6 to 6
- residual: bfloat16 [32, 768, 1024], P(('scene', 'cam')), parts along dimension 0, may hold values from -1.5 to 1.5
- w_out: bfloat16 [1024, 1024], replicated, may hold values from -0.1875 to 0.1875
- neighbours: int32 [32, 4], P(('scene', 'cam')), parts along dimension 0, may hold values from 0 to 15, as said below
- band_start: int32 [32, 4], P(('scene', 'cam')), parts along dimension 0, may hold values from 0 to 3
- band_blocks: int32 [32, 4, 6, 2], P(('scene', 'cam')), parts along dimension 0, may hold values from 0 to 2, as said below
- band_count: int32 [32, 4, 6], P(('scene', 'cam')), parts along dimension 0, may hold values from 1 to 2, as said below
Outputs:
- output: bfloat16 [32, 768, 1024], P(('scene', 'cam')), parts along dimension 0
The draws below stay inside these ranges and needn't reach their ends.
There are 2 independent parts, one for each index of `scene`. The reference program is written for one: setup_inputs(seed, part) draws one part's arguments, and reference() takes and returns one part's arrays. A program takes and returns all parts, laid end to end along the dimension named above; an argument that names none is the same for every part. Nothing has to cross between parts.
Inputs may be any that keep to these rules, and one draw needn't show every extreme that they name: `neighbours`: row v lists the views (v + k) mod 16 for k = 1, -1, 2, -2, each once, in an order drawn for each row. `band_blocks`: each list holds 2 different numbers; entries at positions band_count or later are not read. `band_count`: query block 0 of every slot has 2.
All inputs are finite; a program needn't handle non-finite values.
Results may differ from the reference program's by a relative error of at most 0.008.
Values may be sent and summed in bfloat16 or wider, within the bound.
A program may use at most 128 MiB of HBM per device.

```python
import jax
import jax.numpy as jnp
from jax import lax

D = 1024
HEADS = 16
TOK = 768
MOST = 2
RIGS = 1
VIEWS = 16
QB = 6
WIN = 3


def drawn_pair(key):
    base_key = jax.random.fold_in(key, 17)
    query_key, key_key = jax.random.split(base_key, 2)
    query_draw = 2.0 * jnp.clip(jax.random.normal(query_key, (VIEWS, TOK, D), jnp.float32), -6.0, 6.0)
    key_draw = jnp.clip(jax.random.normal(key_key, (VIEWS, TOK, D), jnp.float32), -6.0, 6.0)
    return (query_draw.astype(jnp.bfloat16), key_draw.astype(jnp.bfloat16))


def draw_queries(key, part):
    return drawn_pair(key)[0]


def draw_keys(key, part):
    return drawn_pair(key)[1]


def draw_neighbours(key, part):
    order_key = jax.random.fold_in(key, 3)
    ranks = jax.random.randint(order_key, (VIEWS, 4), 0, 1 << 20) * 4 + jnp.arange(4, dtype=jnp.int32)[None, :]
    order = jnp.argsort(ranks, axis=1, stable=True)
    offsets = jnp.array([1, -1, 2, -2], dtype=jnp.int32)[order]
    views = jnp.arange(VIEWS, dtype=jnp.int32)[:, None]
    return ((views + offsets * RIGS + 2 * VIEWS) % VIEWS).astype(jnp.int32)


def draw_band_blocks(key, part):
    order_key = jax.random.fold_in(key, 5)
    ranks = jax.random.randint(order_key, (VIEWS, 4, QB, WIN), 0, 1 << 20) * WIN + jnp.arange(WIN, dtype=jnp.int32)
    order = jnp.argsort(ranks, axis=-1, stable=True)
    return order[..., :MOST].astype(jnp.int32)


def draw_band_count(key, part):
    level_key = jax.random.fold_in(key, 7)
    roll_key = jax.random.fold_in(key, 11)
    levels = jax.random.randint(level_key, (VIEWS, 1, 1), 1, 10)
    rolls = jax.random.randint(roll_key, (VIEWS, 4, QB), 0, 10)
    counted = jnp.where(rolls < levels, MOST, 1).astype(jnp.int32)
    return counted.at[:, :, 0].set(MOST)


def plant(values, rng, low, top_value):
    place = [jax.random.randint(jax.random.fold_in(rng, axis), (), 0, length) for axis, length in enumerate(values.shape)]
    main_axis = values.shape.index(max(values.shape))
    neighbour = place[:main_axis] + [(place[main_axis] + 1) % values.shape[main_axis]] + place[main_axis + 1:]
    return values.at[tuple(place)].set(low).at[tuple(neighbour)].set(top_value)


def shard_levels(key, dims, cuts, least, high):
    def one(dim, shards_of):
        draws = jax.random.uniform(jax.random.fold_in(jax.random.fold_in(key, 6), dim), (shards_of,), jnp.float32, least / len(cuts), high / len(cuts))
        return jnp.repeat(jnp.exp(draws), dims[dim] // shards_of).reshape((-1,) + (1,) * (len(dims) - dim - 1))

    level = one(*cuts[0])
    for cut in cuts[1:]:
        level = level * one(*cut)
    return level


def gaussian(stream_key, dims, width, reach, cuts=(), kind=jnp.bfloat16):
    values = width * jax.random.normal(stream_key, dims, jnp.float32)
    if cuts:
        values = values * shard_levels(stream_key, dims, cuts, -0.22, 0.18)
    return jnp.clip(values, -reach, reach).astype(kind)


def setup_inputs(seed: int = 0, part: int = 0) -> dict:
    key_list = jax.random.split(jax.random.key(seed), 10)
    part_keys = jax.random.split(jax.random.fold_in(key_list[9], part), 10)
    queries = draw_queries(jax.random.fold_in(jax.random.fold_in(key_list[9], part), 71), part)
    keys = draw_keys(jax.random.fold_in(jax.random.fold_in(key_list[9], part), 71), part)
    values = gaussian(part_keys[2], (VIEWS, TOK, D), 1.0, 6.0, ((0, 16),))
    residual = gaussian(part_keys[3], (VIEWS, TOK, D), 0.25, 1.5, ((0, 16),))
    w_out = gaussian(key_list[4], (D, D), D ** -0.5, 0.1875)
    neighbours = draw_neighbours(jax.random.fold_in(jax.random.fold_in(key_list[9], part), 71), part)
    band_start = plant(jax.random.randint(part_keys[6], (VIEWS, 4), 0, QB - WIN + 1), jax.random.fold_in(part_keys[6], 1), 0, QB - WIN).astype(jnp.int32)
    band_blocks = draw_band_blocks(jax.random.fold_in(jax.random.fold_in(key_list[9], part), 71), part)
    band_count = draw_band_count(jax.random.fold_in(jax.random.fold_in(key_list[9], part), 71), part)
    return dict(queries=queries, keys=keys, values=values, residual=residual, w_out=w_out, neighbours=neighbours, band_start=band_start, band_blocks=band_blocks, band_count=band_count)


def reference(queries, keys, values, residual, w_out, neighbours, band_start, band_blocks, band_count):
    cameras, tokens, model_width = queries.shape
    qblocks = band_count.shape[2]
    most_blocks = band_blocks.shape[3]
    block_len = tokens // qblocks
    head_dim = model_width // HEADS
    score_scale = 1.0 / (head_dim ** 0.5)
    key_tiles = keys.reshape(cameras, qblocks, block_len, model_width)
    value_tiles = values.reshape(cameras, qblocks, block_len, model_width)

    def one_view(view_index):
        near_cams = neighbours[view_index]
        absolute = band_start[view_index][:, None, None] + band_blocks[view_index]
        near_keys = key_tiles[near_cams[:, None, None], absolute]
        near_values = value_tiles[near_cams[:, None, None], absolute]
        near_keys = jnp.transpose(near_keys, (1, 0, 2, 3, 4)).reshape(qblocks, 4 * most_blocks * block_len, model_width)
        near_values = jnp.transpose(near_values, (1, 0, 2, 3, 4)).reshape(qblocks, 4 * most_blocks * block_len, model_width)
        all_keys = jnp.concatenate([key_tiles[view_index], near_keys], axis=1).reshape(qblocks, -1, HEADS, head_dim)
        all_values = jnp.concatenate([value_tiles[view_index], near_values], axis=1).reshape(qblocks, -1, HEADS, head_dim)
        live_slots = jnp.arange(most_blocks, dtype=jnp.int32)[None, None, :] < band_count[view_index][:, :, None]
        live_slots = jnp.repeat(jnp.transpose(live_slots, (1, 0, 2)), block_len, axis=2).reshape(qblocks, -1)
        visible = jnp.concatenate([jnp.ones((qblocks, block_len), dtype=bool), live_slots], axis=1)
        query_tiles = queries[view_index].reshape(qblocks, block_len, HEADS, head_dim)
        scores = jnp.einsum("gqhd,gkhd->ghqk", query_tiles.astype(jnp.float32), all_keys.astype(jnp.float32)) * score_scale
        scores = jnp.where(visible[:, None, None, :], scores, -jnp.inf)
        row_max = jnp.max(scores, axis=-1, keepdims=True)
        expo_scores = jnp.exp(scores - row_max)
        weights = (expo_scores / jnp.sum(expo_scores, axis=-1, keepdims=True)).astype(jnp.bfloat16)
        attended = jnp.einsum("ghqk,gkhd->gqhd", weights.astype(jnp.float32), all_values.astype(jnp.float32))
        attended = attended.astype(jnp.bfloat16).reshape(tokens, model_width)
        projected = jnp.dot(attended, w_out, preferred_element_type=jnp.float32)
        return (residual[view_index].astype(jnp.float32) + projected).astype(jnp.bfloat16)

    return lax.map(one_view, jnp.arange(cameras, dtype=jnp.int32))
```

```python
import functools
import math

import jax
import jax.numpy as jnp
from jax import lax
from jax.experimental import pallas as pl
from jax.experimental.pallas import tpu as pltpu
from jax.sharding import PartitionSpec as P

HEADS = 16
LANES = 128
ROLES = 4
HIDDEN = -1e30
MESH = pl.DeviceIdType.MESH


def relays(cameras, rigs):
    return rigs == 1 and cameras % 4 == 0


def kernel(cfg, q_hbm, k_hbm, v_hbm, r_hbm, w_hbm, near_ref, start_ref, block_ref, count_ref, out_ref, *scratch):
    cameras, rigs, chunks, qblocks, most, head_dim = cfg
    relay = relays(cameras, rigs)
    take = iter(scratch)
    near = [[[next(take) for _ in range(chunks)] for _ in range(ROLES)] for _ in range(2)]
    q_ref, own_k, own_v, r_ref, w_ref, probs_ref, att_ref, acc_ref, own_sem = [next(take) for _ in range(9)]
    first_send, first_recv, x_send, z_send, b_send, b_recv, x_recv, z_recv = [next(take) for _ in range(8)]
    splits = x_recv.shape[2]
    size = near[0][0][0].shape[0] // splits
    own = (own_k, own_v)
    block_len = q_ref.shape[1]
    heads = LANES // head_dim
    pair = 2 if chunks % 2 == 0 else 1
    part_a, part_b, part_x, part_z = range(ROLES)
    me = lax.axis_index("cam")

    def at(offset):
        return lax.rem(me + offset + 2 * cameras, cameras)

    if relay:
        column = lax.rem(me // 2, 2)
        core = lax.rem(me, 2)
        partner = me + 1 - 2 * core
        across = me + 2 - 4 * column
        z_to = at(4 - 8 * column)
        z_from = at(8 * column - 4)
        from_x = lax.rem(column + core, 2) == 0
        z_view = at(4 * column - 2)
        partner_x = partner + 2 - 4 * column
        partner_z = lax.rem(partner + 4 * column - 2 + cameras, cameras)
        b_view = jnp.where(from_x, partner_z, partner_x)
        views = (partner, b_view, across, z_view)
        peers = (partner, across, z_to, z_from)
        first = ((part_a, partner),)
    else:
        views = (at(rigs), at(-rigs), at(2 * rigs), at(-2 * rigs))
        peers = views
        first = ((part_a, views[1]), (part_b, views[0]), (part_x, views[3]), (part_z, views[2]))

    loads = [
        pltpu.make_async_copy(src, dst, own_sem.at[n])
        for n, (src, dst) in enumerate(
            ((k_hbm, own_k), (v_hbm, own_v), (q_hbm, q_ref), (w_hbm, w_ref), (r_hbm, r_ref))
        )
    ]
    for copy in loads[:2]:
        copy.start()

    barrier = pltpu.get_barrier_semaphore()
    for peer in peers:
        pl.semaphore_signal(barrier, inc=1, device_id={"cam": peer}, device_id_type=MESH)
    pl.semaphore_wait(barrier, len(peers))

    def remote(src, dst, send, recv, target):
        return pltpu.make_async_remote_copy(
            src_ref=src, dst_ref=dst, send_sem=send, recv_sem=recv,
            device_id={"cam": target}, device_id_type=MESH,
        )

    def cols(g):
        return slice(g * LANES, (g + 1) * LANES)

    def some(part):
        return pl.ds(part * size, size)

    def first_copy(lane, g, kind):
        role, target = first[lane]
        return remote(
            own[kind].at[:, :, cols(g)], near[kind][role][g],
            first_send.at[lane, g, kind], first_recv.at[lane, g, kind], target,
        )

    def x_copy(g, kind, part):
        return remote(
            own[kind].at[some(part), :, cols(g)], near[kind][part_x][g].at[some(part)],
            x_send.at[g, kind], x_recv.at[g, kind, part], across,
        )

    def z_copy(g, kind, part):
        return remote(
            near[kind][part_x][g].at[some(part)], near[kind][part_z][g].at[some(part)],
            z_send.at[g, kind], z_recv.at[g, kind, part], z_to,
        )

    def b_copy(g, kind, part, source):
        return remote(
            near[kind][source][g].at[some(part)], near[kind][part_b][g].at[some(part)],
            b_send.at[g, kind], b_recv.at[g, kind], partner,
        )

    def whole(g, kind, send, recv):
        buffer = near[kind][part_b][g]
        return remote(buffer, buffer, send.at[g, kind], recv.at[g, kind], partner)

    def each(body, count=qblocks, unroll=1):
        def step(b, carry):
            body(b)
            return carry

        lax.fori_loop(0, count, step, 0, unroll=unroll)

    slots = []
    for view in views:
        slot = jnp.int32(0)
        for s in range(1, ROLES):
            slot = jnp.where(near_ref[0, s] == view, s, slot)
        slots.append(slot)
    starts = [start_ref[0, slot] for slot in slots]

    def listed(r, b, m):
        index = starts[r] + block_ref[0, slots[r], m, b]
        if m == 0:
            return index, None
        live = m < count_ref[0, slots[r], b]
        return jnp.where(live, index, 0), jnp.where(live, 0.0, HIDDEN)

    def score(g, b):
        q = q_ref[b, :, cols(g)] * jnp.asarray(1.0 / math.sqrt(head_dim), jnp.bfloat16)
        lane = lax.broadcasted_iota(jnp.int32, (block_len, LANES), 1) // head_dim
        q2 = jnp.concatenate([jnp.where(lane == h, q, jnp.zeros_like(q)) for h in range(heads)], axis=0)
        dims = (((1,), (1,)), ((), ()))

        def dot(keys):
            return lax.dot_general(q2, keys, dims, preferred_element_type=jnp.float32)

        scores = [dot(own_k[b, :, cols(g)])]
        for r in range(ROLES):
            found = [listed(r, b, m) for m in range(most)]
            got = dot(jnp.concatenate([near[0][r][g][index] for index, _ in found], axis=0))
            for m, (_, bias) in enumerate(found):
                piece = got[:, m * block_len:(m + 1) * block_len]
                scores.append(piece if bias is None else piece + bias)
        scores = jnp.concatenate(scores, axis=1)
        top = jnp.max(scores, axis=1, keepdims=True)
        expo = jnp.exp(scores - top)
        total = jnp.sum(expo, axis=1, keepdims=True)
        probs_ref[b] = (expo * (1.0 / total)).astype(jnp.bfloat16)

    def mix(g, b):
        lane = lax.broadcasted_iota(jnp.int32, (block_len, LANES), 1) // head_dim
        vals = [own_v[b, :, cols(g)]]
        for r in range(ROLES):
            vals += [near[1][r][g][listed(r, b, m)[0]] for m in range(most)]
        mixed = jnp.dot(probs_ref[b], jnp.concatenate(vals, axis=0), preferred_element_type=jnp.float32)
        result = mixed[:block_len]
        for h in range(1, heads):
            result = jnp.where(lane == h, mixed[h * block_len:(h + 1) * block_len], result)
        half = g % pair
        att_ref[b, :, half * LANES:(half + 1) * LANES] = result.astype(jnp.bfloat16)
        if half == pair - 1:
            rows = slice((g - half) * LANES, (g + 1) * LANES)
            base = r_ref[b].astype(jnp.float32) if g == half else acc_ref[b]
            summed = base + jnp.dot(att_ref[b], w_ref[rows, :], preferred_element_type=jnp.float32)
            if g == chunks - 1:
                out_ref[b] = summed.astype(out_ref.dtype)
            else:
                acc_ref[b] = summed

    for copy in loads[:2]:
        copy.wait()
    if relay:
        for g in range(chunks):
            for kind in range(2):
                each(lambda part: x_copy(g, kind, part).start(), splits)
    for copy in loads[2:]:
        copy.start()
    for lane in range(len(first)):
        for g in range(chunks):
            for kind in range(2):
                first_copy(lane, g, kind).start()

    def first_wait(g, kind):
        for lane in range(len(first)):
            first_copy(lane, g, kind).wait_recv()

    if relay:

        def after_x(g, kind, part):
            x_copy(g, kind, part).wait_recv()
            z_copy(g, kind, part).start()

            @pl.when(from_x)
            def _():
                b_copy(g, kind, part, part_x).start()

        def after_z(g, kind, part):
            z_copy(g, kind, part).wait_recv()

            @pl.when(jnp.logical_not(from_x))
            def _():
                b_copy(g, kind, part, part_z).start()

        def arrive(g, kind):
            first_wait(g, kind)
            whole(g, kind, b_send, b_recv).wait_recv()

        def drain(g, kind):
            for send in (x_send, z_send, b_send):
                whole(g, kind, send, b_recv).wait_send()

        for step in range(chunks + 2):
            if step == 1:
                for copy in loads[2:]:
                    copy.wait()
            for kind in range(2):
                work, done = (mix, step - 2) if kind == 0 else (score, step - 1)
                live = 0 <= done < chunks
                if live:
                    arrive(done, 1 - kind)
                if step > chunks:
                    if live:
                        each(lambda b: work(done, b), unroll=LAST if qblocks % LAST == 0 else 1)
                    continue

                def body(part):
                    if step < chunks:
                        after_x(step, kind, part)
                    if 1 <= step <= chunks:
                        after_z(step - 1, kind, part)
                    if live:
                        each(lambda b: work(done, part * size + b), size)

                each(body, splits)
                if 0 <= step - 3 < chunks - 2:
                    drain(step - 3, kind)

        for g in range(max(0, chunks - 2), chunks):
            for kind in range(2):
                drain(g, kind)
    else:
        for copy in loads[2:]:
            copy.wait()
        for g in range(chunks):
            first_wait(g, 0)
            each(lambda b: score(g, b))
            first_wait(g, 1)
            each(lambda b: mix(g, b))
    for lane in range(len(first)):
        for g in range(chunks):
            for kind in range(2):
                first_copy(lane, g, kind).wait_send()


def per_device(queries, keys, values, residual, w_out, neighbours, band_start, band_blocks, band_count):
    tokens, width = queries.shape[1:]
    qblocks = band_count.shape[2]
    most = band_blocks.shape[3]
    cameras = lax.axis_size("cam")
    rigs = cameras // min(32, cameras)
    chunks = width // LANES
    head_dim = width // HEADS
    cfg = (cameras, rigs, chunks, qblocks, most, head_dim)
    relay = relays(cameras, rigs)
    lanes = 1 if relay else ROLES
    dma = pltpu.SemaphoreType.DMA
    anywhere = pl.BlockSpec(memory_space=pltpu.HBM)
    scalars = pl.BlockSpec(memory_space=pltpu.SMEM)
    block_len = tokens // qblocks
    blocks = (qblocks, block_len, width)
    part = (qblocks, block_len, LANES)
    heads = LANES // head_dim
    pair = 2 if chunks % 2 == 0 else 1
    splits = math.gcd(SPLITS, qblocks)
    bf16 = jnp.bfloat16
    out = pl.pallas_call(
        functools.partial(kernel, cfg),
        out_shape=pltpu.VMEM(blocks, bf16),
        in_specs=[anywhere] * 5 + [scalars] * 4,
        out_specs=pl.BlockSpec(memory_space=pltpu.VMEM),
        scratch_shapes=[pltpu.VMEM(part, bf16)] * (2 * ROLES * chunks)
        + [pltpu.VMEM(blocks, bf16)] * 4
        + [
            pltpu.VMEM((width, width), bf16),
            pltpu.VMEM((qblocks, heads * block_len, (1 + ROLES * most) * block_len), bf16),
            pltpu.VMEM((qblocks, block_len, pair * LANES), bf16),
            pltpu.VMEM(blocks, jnp.float32),
            dma((5,)),
            dma((lanes, chunks, 2)),
            dma((lanes, chunks, 2)),
        ]
        + [dma((chunks, 2) if relay else (1, 1))] * 4
        + [dma((chunks, 2, splits) if relay else (1, 1, 1))] * 2,
        compiler_params=pltpu.CompilerParams(
            collective_id=0, has_side_effects=True, vmem_limit_bytes=VMEM_LIMIT * 1024 * 1024
        ),
        name="band_attention",
    )(
        *(x[0].reshape(blocks) for x in (queries, keys, values, residual)),
        w_out, neighbours, band_start, jnp.swapaxes(band_blocks, 2, 3), band_count,
    )
    return out.reshape(tokens, width)[None]


VMEM_LIMIT = 62
SPLITS = 3
LAST = 3


def solution(mesh):
    rows = ("scene", "cam")
    return jax.shard_map(
        per_device,
        mesh=mesh,
        in_specs=(
            P(rows, None, None),
            P(rows, None, None),
            P(rows, None, None),
            P(rows, None, None),
            P(),
            P(rows, None),
            P(rows, None),
            P(rows, None, None, None),
            P(rows, None, None),
        ),
        out_specs=P(rows, None, None),
        check_vma=False,
    )
```

```python
import functools
import math

import jax
import jax.numpy as jnp
from jax import lax
from jax.experimental import pallas as pl
from jax.experimental.pallas import tpu as pltpu
from jax.sharding import PartitionSpec as P

HEADS = 16
LANES = 128
ROLES = 4
WIN = 3
HIDDEN = -1e30
MESH = pl.DeviceIdType.MESH


def relays(cameras, rigs):
    return rigs == 1 and cameras % 4 == 0


def cuts(cfg, role, g, kind):
    cameras, rigs, chunks = cfg[:3]
    if role != 2 or not relays(cameras, rigs) or g < chunks - 1:
        return 1
    return CUTS[kind]


def kernel(cfg, q_hbm, k_hbm, v_hbm, r_hbm, w_hbm, near_ref, start_ref, block_ref, count_ref, out_ref, *scratch):
    cameras, rigs, chunks, qblocks, most, head_dim = cfg
    relay = relays(cameras, rigs)
    take = iter(scratch)
    part_a, part_b, part_x, part_z = range(ROLES)
    near = [
        [[[next(take) for _ in range(cuts(cfg, role, g, kind))] for g in range(chunks)] for role in range(ROLES)]
        for kind in range(2)
    ]
    q_ref, own_k, own_v, r_ref, w_ref, probs_ref, att_ref, acc_ref, own_sem = [next(take) for _ in range(9)]
    first_send, first_recv = next(take), next(take)
    if relay:
        near_sem, far_sem, told_near, told_start, tell_send, tell_recv = [next(take) for _ in range(6)]
        x_send, z_send, b_send, z_recv, b_recv, x_recv = [next(take) for _ in range(6)]
        staged = [
            [[[next(take) for _ in range(2)] for _ in range(cuts(cfg, part_x, g, kind))] for g in range(chunks)]
            for kind in range(2)
        ]
    own = (own_k, own_v)
    block_len = q_ref.shape[1]
    heads = LANES // head_dim
    pair = 2 if chunks % 2 == 0 else 1
    me = lax.axis_index("cam")

    def at(offset):
        return lax.rem(me + offset + 2 * cameras, cameras)

    if relay:
        column = lax.rem(me // 2, 2)
        core = lax.rem(me, 2)
        partner = me + 1 - 2 * core
        across = me + 2 - 4 * column
        z_to = at(4 - 8 * column)
        z_from = at(8 * column - 4)
        from_x = lax.rem(column + core, 2) == 0
        z_view = at(4 * column - 2)
        partner_x = partner + 2 - 4 * column
        partner_z = lax.rem(partner + 4 * column - 2 + cameras, cameras)
        b_view = jnp.where(from_x, partner_z, partner_x)
        views = (partner, b_view, across, z_view)
        first = ((part_a, partner),)
    else:
        views = (at(rigs), at(-rigs), at(2 * rigs), at(-2 * rigs))
        first = ((part_a, views[1]), (part_b, views[0]), (part_x, views[3]), (part_z, views[2]))

    loads = [
        pltpu.make_async_copy(src, dst, own_sem.at[n])
        for n, (src, dst) in enumerate(
            ((k_hbm, own_k), (v_hbm, own_v), (q_hbm, q_ref), (w_hbm, w_ref), (r_hbm, r_ref))
        )
    ]
    for copy in loads[:2]:
        copy.start()

    def signal(sem, peer):
        pl.semaphore_signal(sem, inc=1, device_id={"cam": peer}, device_id_type=MESH)

    barrier = pltpu.get_barrier_semaphore()
    if relay:
        signal(barrier, across - core)
        signal(barrier, z_from + 1 - core)
        signal(barrier, z_to + 1 - core)

        @pl.when(core == 1)
        def _():
            signal(barrier, partner)

        @pl.when(core == 0)
        def _():
            pl.semaphore_wait(barrier, 3)
            signal(near_sem, partner)

        @pl.when(core == 1)
        def _():
            pl.semaphore_wait(near_sem, 1)
    else:
        for view in views:
            signal(barrier, view)
        pl.semaphore_wait(barrier, len(views))

    def remote(src, dst, send, recv, target):
        return pltpu.make_async_remote_copy(
            src_ref=src, dst_ref=dst, send_sem=send, recv_sem=recv,
            device_id={"cam": target}, device_id_type=MESH,
        )

    def cols(g):
        return slice(g * LANES, (g + 1) * LANES)

    def first_copy(lane, g, kind):
        role, target = first[lane]
        return remote(
            own[kind].at[:, :, cols(g)], near[kind][role][g][0],
            first_send.at[lane, g, kind], first_recv.at[lane, g, kind], target,
        )

    def rows(g, kind, part):
        size = block_len // cuts(cfg, part_x, g, kind)
        return pl.ds(part * size, size)

    def x_copy(g, kind, part):
        source = own if g else (k_hbm, v_hbm)
        return remote(
            source[kind].at[:, rows(g, kind, part), cols(g)], near[kind][part_x][g][part],
            x_send.at[g, kind], x_recv.at[g, kind, part], across,
        )

    def z_copy(g, kind, part):
        return remote(
            staged[kind][g][part][0], near[kind][part_z][g][0].at[:, rows(g, kind, part)],
            z_send.at[g, kind], z_recv.at[g, kind], z_to,
        )

    def far_copy(g, kind, part):
        return remote(
            staged[kind][g][part][1], near[kind][part_b][g][0].at[pl.ds(0, WIN), rows(g, kind, part)],
            b_send.at[g, kind], b_recv.at[g, kind], z_to + 1 - 2 * core,
        )

    def near_copy(g, kind, part):
        return remote(
            near[kind][part_x][g][part], near[kind][part_b][g][0].at[:, rows(g, kind, part)],
            b_send.at[g, kind], b_recv.at[g, kind], partner,
        )

    def whole(g, kind, role, send, recv):
        buffer = near[kind][role][g][0]
        return remote(buffer, buffer, send.at[g, kind], recv.at[g, kind], partner)

    def each(body, count=qblocks, unroll=1):
        def step(b, carry):
            body(b)
            return carry

        lax.fori_loop(0, count, step, 0, unroll=unroll)

    slots = []
    for view in views:
        slot = jnp.int32(0)
        for s in range(1, ROLES):
            slot = jnp.where(near_ref[0, s] == view, s, slot)
        slots.append(slot)
    starts = [start_ref[0, slot] for slot in slots]
    if relay:
        starts[part_z] = jnp.int32(0)
        starts[part_b] = jnp.where(from_x, 0, starts[part_b])

    def listed(r, b, m):
        index = starts[r] + block_ref[0, slots[r], m, b]
        if m == 0:
            return index, None
        live = m < count_ref[0, slots[r], b]
        return jnp.where(live, index, 0), jnp.where(live, 0.0, HIDDEN)

    def score(g, b):
        q = q_ref[b, :, cols(g)] * jnp.asarray(1.0 / math.sqrt(head_dim), jnp.bfloat16)
        lane = lax.broadcasted_iota(jnp.int32, (block_len, LANES), 1) // head_dim
        q2 = jnp.concatenate([jnp.where(lane == h, q, jnp.zeros_like(q)) for h in range(heads)], axis=0)
        dims = (((1,), (1,)), ((), ()))

        def dot(keys):
            return lax.dot_general(q2, keys, dims, preferred_element_type=jnp.float32)

        scores = [dot(own_k[b, :, cols(g)])]
        for r in range(ROLES):
            found = [listed(r, b, m) for m in range(most)]
            got = dot(jnp.concatenate([part[index] for index, _ in found for part in near[0][r][g]], axis=0))
            for m, (_, bias) in enumerate(found):
                piece = got[:, m * block_len:(m + 1) * block_len]
                scores.append(piece if bias is None else piece + bias)
        scores = jnp.concatenate(scores, axis=1)
        top = jnp.max(scores, axis=1, keepdims=True)
        expo = jnp.exp(scores - top)
        total = jnp.sum(expo, axis=1, keepdims=True)
        probs_ref[b] = (expo * (1.0 / total)).astype(jnp.bfloat16)

    def mix(g, b):
        lane = lax.broadcasted_iota(jnp.int32, (block_len, LANES), 1) // head_dim
        vals = [own_v[b, :, cols(g)]]
        for r in range(ROLES):
            vals += [part[listed(r, b, m)[0]] for m in range(most) for part in near[1][r][g]]
        mixed = jnp.dot(probs_ref[b], jnp.concatenate(vals, axis=0), preferred_element_type=jnp.float32)
        result = mixed[:block_len]
        for h in range(1, heads):
            result = jnp.where(lane == h, mixed[h * block_len:(h + 1) * block_len], result)
        half = g % pair
        att_ref[b, :, half * LANES:(half + 1) * LANES] = result.astype(jnp.bfloat16)
        if half == pair - 1:
            rows = slice((g - half) * LANES, (g + 1) * LANES)
            base = r_ref[b].astype(jnp.float32) if g == half else acc_ref[b]
            summed = base + jnp.dot(att_ref[b], w_ref[rows, :], preferred_element_type=jnp.float32)
            if g == chunks - 1:
                out_ref[b] = summed.astype(out_ref.dtype)
            else:
                acc_ref[b] = summed

    parts = [(g, kind, part) for g in range(chunks) for kind in range(2) for part in range(cuts(cfg, part_x, g, kind))]
    if relay:
        for g, kind, part in parts:
            if g == 0:
                x_copy(g, kind, part).start()
    for copy in loads[:2]:
        copy.wait()
    if relay:
        for g, kind, part in parts:
            if g > 0:
                x_copy(g, kind, part).start()
    for copy in loads[2:]:
        copy.start()
    for lane in range(len(first)):
        for g in range(chunks):
            for kind in range(2):
                first_copy(lane, g, kind).start()

    def first_wait(g, kind):
        for lane in range(len(first)):
            first_copy(lane, g, kind).wait_recv()

    if relay:

        @pl.when(core == 1)
        def _():
            pl.semaphore_wait(barrier, 4)
            signal(far_sem, partner)

        @pl.when(core == 0)
        def _():
            pl.semaphore_wait(far_sem, 1)

        def tell(n, k):
            row, place = ((near_ref, told_near), (start_ref, told_start))[k]
            return remote(row, place.at[core], tell_send.at[n, k], tell_recv.at[core, k], z_from - core + n)

        def told(n, view):
            start = told_start[n, 0, 0]
            for s in range(1, ROLES):
                start = jnp.where(told_near[n, 0, s] == view, told_start[n, 0, s], start)
            return start

        for n in range(2):
            for k in range(2):
                tell(n, k).start()
        for n in range(2):
            for k in range(2):
                tell(n, k).wait_send()
        for n in range(2):
            for k in range(2):
                remote(
                    told_near.at[n], (told_near, told_start)[k].at[n], tell_send.at[n, k], tell_recv.at[n, k], partner
                ).wait_recv()
        start_z = told(core, across)
        start_b = told(1 - core, across)

        def relay_part(g, kind, part):
            x_copy(g, kind, part).wait_recv()
            source = near[kind][part_x][g][part]
            for n in range(WIN):
                staged[kind][g][part][0][n] = source[start_z + n]
            z_copy(g, kind, part).start()

            @pl.when(from_x)
            def _():
                near_copy(g, kind, part).start()

            @pl.when(jnp.logical_not(from_x))
            def _():
                for n in range(WIN):
                    staged[kind][g][part][1][n] = source[start_b + n]
                far_copy(g, kind, part).start()

        def arrive(g, kind):
            first_wait(g, kind)

            @pl.when(from_x)
            def _():
                whole(g, kind, part_z, b_send, b_recv).wait_recv()

            @pl.when(jnp.logical_not(from_x))
            def _():
                whole(g, kind, part_b, b_send, b_recv).wait_recv()

            whole(g, kind, part_z, z_send, z_recv).wait_recv()

        def drain(g, kind):
            whole(g, kind, part_b, x_send, b_recv).wait_send()
            whole(g, kind, part_z, z_send, b_recv).wait_send()

            @pl.when(from_x)
            def _():
                whole(g, kind, part_b, b_send, b_recv).wait_send()

            @pl.when(jnp.logical_not(from_x))
            def _():
                whole(g, kind, part_z, b_send, b_recv).wait_send()

        def run(work, g, kind, low, high, unroll=2):
            if low == 0:
                arrive(g, kind)
            count = high - low
            each(lambda b: work(g, low + b), count, unroll if count % unroll == 0 else 1)

        end = chunks - 1
        for g, kind, part in parts:
            relay_part(g, kind, part)
            if g == 1 and kind == 0 and part == 0:
                for copy in loads[2:]:
                    copy.wait()
            if g == 0:
                continue
            if g < end:
                run((score, mix)[kind], g - 1, kind, 0, qblocks)
                if g >= 2:
                    drain(g - 2, kind)
            elif kind == 0:
                n = cuts(cfg, part_x, g, kind)
                run(score, g - 1, 0, part * qblocks // n, (part + 1) * qblocks // n, 3)
            elif part >= cuts(cfg, part_x, g, kind) - 2:
                n = part - cuts(cfg, part_x, g, kind) + 2
                run(mix, g - 1, 1, n * qblocks // 2, (n + 1) * qblocks // 2, 3)
        run(score, end, 0, 0, qblocks)
        run(mix, end, 1, 0, qblocks, LAST)
        for g in range(max(0, end - 2), chunks):
            for kind in range(2):
                drain(g, kind)
    else:
        for copy in loads[2:]:
            copy.wait()
        for g in range(chunks):
            first_wait(g, 0)
            each(lambda b: score(g, b), qblocks)
            first_wait(g, 1)
            each(lambda b: mix(g, b), qblocks)
    for lane in range(len(first)):
        for g in range(chunks):
            for kind in range(2):
                first_copy(lane, g, kind).wait_send()


def per_device(queries, keys, values, residual, w_out, neighbours, band_start, band_blocks, band_count):
    tokens, width = queries.shape[1:]
    qblocks = band_count.shape[2]
    most = band_blocks.shape[3]
    cameras = lax.axis_size("cam")
    rigs = cameras // min(32, cameras)
    chunks = width // LANES
    head_dim = width // HEADS
    cfg = (cameras, rigs, chunks, qblocks, most, head_dim)
    relay = relays(cameras, rigs)
    lanes = 1 if relay else ROLES
    dma = pltpu.SemaphoreType.DMA
    anywhere = pl.BlockSpec(memory_space=pltpu.HBM)
    scalars = pl.BlockSpec(memory_space=pltpu.SMEM)
    block_len = tokens // qblocks
    blocks = (qblocks, block_len, width)
    heads = LANES // head_dim
    pair = 2 if chunks % 2 == 0 else 1
    bf16 = jnp.bfloat16
    regular = pltpu.SemaphoreType.REGULAR
    scratch = []
    for kind in range(2):
        for role in range(ROLES):
            for g in range(chunks):
                n = cuts(cfg, role, g, kind)
                count = WIN if relay and role == 3 else qblocks
                scratch += [pltpu.VMEM((count, block_len // n, LANES), bf16)] * n
    scratch += [pltpu.VMEM(blocks, bf16)] * 4 + [
        pltpu.VMEM((width, width), bf16),
        pltpu.VMEM((qblocks, heads * block_len, (1 + ROLES * most) * block_len), bf16),
        pltpu.VMEM((qblocks, block_len, pair * LANES), bf16),
        pltpu.VMEM(blocks, jnp.float32),
        dma((5,)),
        dma((lanes, chunks, 2)),
        dma((lanes, chunks, 2)),
    ]
    if relay:
        scratch += [regular, regular, pltpu.SMEM((2, 1, ROLES), jnp.int32), pltpu.SMEM((2, 1, ROLES), jnp.int32), dma((2, 2)), dma((2, 2))]
        scratch += [dma((chunks, 2))] * 5 + [dma((chunks, 2, max(CUTS)))]
        for kind in range(2):
            for g in range(chunks):
                n = cuts(cfg, 2, g, kind)
                scratch += [pltpu.VMEM((WIN, block_len // n, LANES), bf16)] * (2 * n)
    out = pl.pallas_call(
        functools.partial(kernel, cfg),
        out_shape=pltpu.VMEM(blocks, bf16),
        in_specs=[anywhere] * 5 + [scalars] * 4,
        out_specs=pl.BlockSpec(memory_space=pltpu.VMEM),
        scratch_shapes=scratch,
        compiler_params=pltpu.CompilerParams(
            collective_id=0, has_side_effects=True, vmem_limit_bytes=VMEM_LIMIT * 1024 * 1024
        ),
        name="band_attention",
    )(
        *(x[0].reshape(blocks) for x in (queries, keys, values, residual)),
        w_out, neighbours, band_start, jnp.swapaxes(band_blocks, 2, 3), band_count,
    )
    return out.reshape(tokens, width)[None]


VMEM_LIMIT = 62
CUTS = (2, 4)
LAST = 3


def solution(mesh):
    rows = ("scene", "cam")
    return jax.shard_map(
        per_device,
        mesh=mesh,
        in_specs=(
            P(rows, None, None),
            P(rows, None, None),
            P(rows, None, None),
            P(rows, None, None),
            P(),
            P(rows, None),
            P(rows, None),
            P(rows, None, None, None),
            P(rows, None, None),
        ),
        out_specs=P(rows, None, None),
        check_vma=False,
    )
```

```python
import functools
import math

import jax
import jax.numpy as jnp
from jax import lax
from jax.experimental import pallas as pl
from jax.experimental.pallas import tpu as pltpu
from jax.sharding import PartitionSpec as P

HEADS = 16
LANES = 128
ROLES = 4
WIN = 3
X_ROLE = 1
HIDDEN = -1e30
MESH = pl.DeviceIdType.MESH


def relays(cameras, rigs):
    return rigs == 1 and cameras % 4 == 0


def cuts(cfg, role, g, kind):
    cameras, rigs, chunks = cfg[:3]
    if role != X_ROLE or not relays(cameras, rigs) or g < chunks - 1:
        return (1,)
    return CUTS[kind]


def kernel(cfg, q_hbm, k_hbm, v_hbm, r_hbm, w_hbm, near_ref, start_ref, block_ref, count_ref, out_ref, *scratch):
    cameras, rigs, chunks, qblocks, most, head_dim = cfg
    relay = relays(cameras, rigs)
    take = iter(scratch)
    part_a, part_x, part_b, part_z = range(ROLES)
    near = [
        [[[next(take) for _ in cuts(cfg, role, g, kind)] for g in range(chunks)] for role in range(ROLES)]
        for kind in range(2)
    ]
    q_ref, own_k, own_v, r_ref, w_ref, probs_ref, att_ref, acc_ref, own_sem = [next(take) for _ in range(9)]
    first_send, first_recv = next(take), next(take)
    if relay:
        mixed_ref, near_sem, far_sem, told_near, told_start, tell_send, tell_recv = [next(take) for _ in range(7)]
        x_send, z_send, b_send, z_recv, b_recv, x_recv = [next(take) for _ in range(6)]
        staged = [
            [[[next(take) for _ in range(2)] for _ in cuts(cfg, part_x, g, kind)] for g in range(chunks)]
            for kind in range(2)
        ]
    own = (own_k, own_v)
    block_len = q_ref.shape[1]
    heads = LANES // head_dim
    pair = 2 if chunks % 2 == 0 else 1
    me = lax.axis_index("cam")

    def at(offset):
        return lax.rem(me + offset + 2 * cameras, cameras)

    if relay:
        column = lax.rem(me // 2, 2)
        core = lax.rem(me, 2)
        partner = me + 1 - 2 * core
        across = me + 2 - 4 * column
        z_to = at(4 - 8 * column)
        z_from = at(8 * column - 4)
        from_x = lax.rem(column + core, 2) == 0
        z_view = at(4 * column - 2)
        partner_x = partner + 2 - 4 * column
        partner_z = lax.rem(partner + 4 * column - 2 + cameras, cameras)
        b_view = jnp.where(from_x, partner_z, partner_x)
        views = (partner, across, b_view, z_view)
        first = ((part_a, partner),)
    else:
        views = (at(rigs), at(-rigs), at(2 * rigs), at(-2 * rigs))
        first = ((0, views[1]), (1, views[0]), (2, views[3]), (3, views[2]))

    loads = [
        pltpu.make_async_copy(src, dst, own_sem.at[n])
        for n, (src, dst) in enumerate(
            ((k_hbm, own_k), (v_hbm, own_v), (q_hbm, q_ref), (w_hbm, w_ref), (r_hbm, r_ref))
        )
    ]
    for copy in loads[:2]:
        copy.start()

    def signal(sem, peer):
        pl.semaphore_signal(sem, inc=1, device_id={"cam": peer}, device_id_type=MESH)

    barrier = pltpu.get_barrier_semaphore()
    if relay:
        signal(barrier, across - core)
        signal(barrier, z_from + 1 - core)
        signal(barrier, z_to + 1 - core)

        @pl.when(core == 1)
        def _():
            signal(barrier, partner)

        @pl.when(core == 0)
        def _():
            pl.semaphore_wait(barrier, 3)
            signal(near_sem, partner)

        @pl.when(core == 1)
        def _():
            pl.semaphore_wait(near_sem, 1)
    else:
        for view in views:
            signal(barrier, view)
        pl.semaphore_wait(barrier, len(views))

    def remote(src, dst, send, recv, target):
        return pltpu.make_async_remote_copy(
            src_ref=src, dst_ref=dst, send_sem=send, recv_sem=recv,
            device_id={"cam": target}, device_id_type=MESH,
        )

    def cols(g):
        return slice(g * LANES, (g + 1) * LANES)

    def first_copy(lane, g, kind):
        role, target = first[lane]
        return remote(
            own[kind].at[:, :, cols(g)], near[kind][role][g][0],
            first_send.at[lane, g, kind], first_recv.at[lane, g, kind], target,
        )

    def rows(g, kind, part):
        sizes = [block_len // n for n in cuts(cfg, part_x, g, kind)]
        return pl.ds(sum(sizes[:part]), sizes[part])

    def x_copy(g, kind, part):
        source = own if g else (k_hbm, v_hbm)
        return remote(
            source[kind].at[:, rows(g, kind, part), cols(g)], near[kind][part_x][g][part],
            x_send.at[g, kind], x_recv.at[g, kind, part], across,
        )

    def z_copy(g, kind, part):
        return remote(
            staged[kind][g][part][0], near[kind][part_z][g][0].at[:, rows(g, kind, part)],
            z_send.at[g, kind], z_recv.at[g, kind], z_to,
        )

    def far_copy(g, kind, part):
        return remote(
            staged[kind][g][part][1], near[kind][part_b][g][0].at[pl.ds(0, WIN), rows(g, kind, part)],
            b_send.at[g, kind], b_recv.at[g, kind], z_to + 1 - 2 * core,
        )

    def near_copy(g, kind, part):
        return remote(
            near[kind][part_x][g][part], near[kind][part_b][g][0].at[:, rows(g, kind, part)],
            b_send.at[g, kind], b_recv.at[g, kind], partner,
        )

    def whole(g, kind, role, send, recv):
        buffer = near[kind][role][g][0]
        return remote(buffer, buffer, send.at[g, kind], recv.at[g, kind], partner)

    def each(body, count=qblocks, unroll=1):
        def step(b, carry):
            body(b)
            return carry

        lax.fori_loop(0, count, step, 0, unroll=unroll)

    slots = []
    for view in views:
        slot = jnp.int32(0)
        for s in range(1, ROLES):
            slot = jnp.where(near_ref[0, s] == view, s, slot)
        slots.append(slot)
    starts = [start_ref[0, slot] for slot in slots]
    if relay:
        starts[part_z] = jnp.int32(0)
        starts[part_b] = jnp.where(from_x, 0, starts[part_b])

    def listed(r, b, m):
        index = starts[r] + block_ref[0, slots[r], m, b]
        if m == 0:
            return index, None
        live = m < count_ref[0, slots[r], b]
        return jnp.where(live, index, 0), jnp.where(live, 0.0, HIDDEN)

    def score(g, b):
        q = q_ref[b, :, cols(g)] * jnp.asarray(1.0 / math.sqrt(head_dim), jnp.bfloat16)
        lane = lax.broadcasted_iota(jnp.int32, (block_len, LANES), 1) // head_dim
        q2 = jnp.concatenate([jnp.where(lane == h, q, jnp.zeros_like(q)) for h in range(heads)], axis=0)
        dims = (((1,), (1,)), ((), ()))

        def dot(keys):
            return lax.dot_general(q2, keys, dims, preferred_element_type=jnp.float32)

        scores = [dot(own_k[b, :, cols(g)])]
        for r in range(ROLES):
            found = [listed(r, b, m) for m in range(most)]
            got = dot(jnp.concatenate([part[index] for index, _ in found for part in near[0][r][g]], axis=0))
            for m, (_, bias) in enumerate(found):
                piece = got[:, m * block_len:(m + 1) * block_len]
                scores.append(piece if bias is None else piece + bias)
        scores = jnp.concatenate(scores, axis=1)
        top = jnp.max(scores, axis=1, keepdims=True)
        expo = jnp.exp(scores - top)
        total = jnp.sum(expo, axis=1, keepdims=True)
        probs_ref[b] = (expo * (1.0 / total)).astype(jnp.bfloat16)

    def weigh(g, b, roles):
        vals = []
        for r in roles:
            if r < 0:
                vals.append(own_v[b, :, cols(g)])
            else:
                vals += [part[listed(r, b, m)[0]] for m in range(most) for part in near[1][r][g]]
        low = 0 if roles[0] < 0 else (1 + roles[0] * most) * block_len
        high = (1 + (roles[-1] + 1) * most) * block_len
        return jnp.dot(probs_ref[b, :, low:high], jnp.concatenate(vals, axis=0), preferred_element_type=jnp.float32)

    def early(g, b):
        mixed_ref[b] = weigh(g, b, (-1, part_a, part_x))

    def late(g, b):
        finish(g, b, mixed_ref[b] + weigh(g, b, (part_b, part_z)))

    def mix(g, b):
        finish(g, b, weigh(g, b, tuple(range(-1, ROLES))))

    def finish(g, b, mixed):
        lane = lax.broadcasted_iota(jnp.int32, (block_len, LANES), 1) // head_dim
        result = mixed[:block_len]
        for h in range(1, heads):
            result = jnp.where(lane == h, mixed[h * block_len:(h + 1) * block_len], result)
        half = g % pair
        place = pl.ds(pl.multiple_of(b * block_len, block_len), block_len)
        att_ref[place, half * LANES:(half + 1) * LANES] = result.astype(jnp.bfloat16)

    def project(g, group, count):
        half = g % pair
        if half < pair - 1:
            return
        place = pl.ds(pl.multiple_of(group * count * block_len, block_len), count * block_len)
        rows = slice((g - half) * LANES, (g + 1) * LANES)
        added = jnp.dot(att_ref[place, :], w_ref[rows, :], preferred_element_type=jnp.float32)
        for n in range(count):
            b = group * count + n
            base = r_ref[b].astype(jnp.float32) if g == half else acc_ref[b]
            summed = base + added[n * block_len:(n + 1) * block_len]
            if g == chunks - 1:
                out_ref[b] = summed.astype(out_ref.dtype)
            else:
                acc_ref[b] = summed

    def project_all(g):
        count = GROUP if qblocks % GROUP == 0 else 1
        each(lambda group: project(g, group, count), qblocks // count)

    parts = [(g, kind, part) for g in range(chunks) for kind in range(2) for part in range(len(cuts(cfg, part_x, g, kind)))]
    if relay:
        for g, kind, part in parts:
            if g == 0:
                x_copy(g, kind, part).start()
    for copy in loads[:2]:
        copy.wait()
    if relay:
        for g, kind, part in parts:
            if g > 0:
                x_copy(g, kind, part).start()
    for copy in loads[2:]:
        copy.start()
    for lane in range(len(first)):
        for g in range(chunks):
            for kind in range(2):
                first_copy(lane, g, kind).start()

    def first_wait(g, kind):
        for lane in range(len(first)):
            first_copy(lane, g, kind).wait_recv()

    if relay:

        @pl.when(core == 1)
        def _():
            pl.semaphore_wait(barrier, 4)
            signal(far_sem, partner)

        @pl.when(core == 0)
        def _():
            pl.semaphore_wait(far_sem, 1)

        def tell(n, k):
            row, place = ((near_ref, told_near), (start_ref, told_start))[k]
            return remote(row, place.at[core], tell_send.at[n, k], tell_recv.at[core, k], z_from - core + n)

        def told(n, view):
            start = told_start[n, 0, 0]
            for s in range(1, ROLES):
                start = jnp.where(told_near[n, 0, s] == view, told_start[n, 0, s], start)
            return start

        for n in range(2):
            for k in range(2):
                tell(n, k).start()
        for n in range(2):
            for k in range(2):
                tell(n, k).wait_send()
        for n in range(2):
            for k in range(2):
                remote(
                    told_near.at[n], (told_near, told_start)[k].at[n], tell_send.at[n, k], tell_recv.at[n, k], partner
                ).wait_recv()
        start_z = told(core, across)
        start_b = told(1 - core, across)

        def relay_part(g, kind, part):
            x_copy(g, kind, part).wait_recv()
            source = near[kind][part_x][g][part]
            for n in range(WIN):
                staged[kind][g][part][0][n] = source[start_z + n]
            z_copy(g, kind, part).start()

            @pl.when(from_x)
            def _():
                near_copy(g, kind, part).start()

            @pl.when(jnp.logical_not(from_x))
            def _():
                for n in range(WIN):
                    staged[kind][g][part][1][n] = source[start_b + n]
                far_copy(g, kind, part).start()

        def arrive(g, kind, all_roles=True):
            if all_roles:
                first_wait(g, kind)

            @pl.when(from_x)
            def _():
                whole(g, kind, part_z, b_send, b_recv).wait_recv()

            @pl.when(jnp.logical_not(from_x))
            def _():
                whole(g, kind, part_b, b_send, b_recv).wait_recv()

            whole(g, kind, part_z, z_send, z_recv).wait_recv()

        def drain(g, kind):
            whole(g, kind, part_b, x_send, b_recv).wait_send()
            whole(g, kind, part_z, z_send, b_recv).wait_send()

            @pl.when(from_x)
            def _():
                whole(g, kind, part_b, b_send, b_recv).wait_send()

            @pl.when(jnp.logical_not(from_x))
            def _():
                whole(g, kind, part_z, b_send, b_recv).wait_send()

        def run(work, g, kind, low, high, unroll=2):
            if low == 0:
                arrive(g, kind)
            count = high - low
            each(lambda b: work(g, low + b), count, unroll if count % unroll == 0 else 1)
            if work is mix and high == qblocks:
                project_all(g)

        end = chunks - 1
        for g, kind, part in parts:
            relay_part(g, kind, part)
            if g == 1 and kind == 0 and part == 0:
                for copy in loads[2:]:
                    copy.wait()
            if g == 0:
                continue
            if g < end:
                run((score, mix)[kind], g - 1, kind, 0, qblocks)
                if g >= 2:
                    drain(g - 2, kind)
            elif kind == 0:
                n = len(cuts(cfg, part_x, g, kind))
                run(score, g - 1, 0, part * qblocks // n, (part + 1) * qblocks // n, 3)
            elif part >= len(cuts(cfg, part_x, g, kind)) - 2:
                n = part - len(cuts(cfg, part_x, g, kind)) + 2
                run(mix, g - 1, 1, n * qblocks // 2, (n + 1) * qblocks // 2, 3)
        run(score, end, 0, 0, qblocks)
        first_wait(end, 1)
        each(lambda b: early(end, b), qblocks, LAST)
        arrive(end, 1, False)
        count = TAIL if qblocks % TAIL == 0 else 1

        def close(group):
            for n in range(count):
                late(end, group * count + n)
            project(end, group, count)

        each(close, qblocks // count, TAIL_UNROLL)
        for g in range(max(0, end - 2), chunks):
            for kind in range(2):
                drain(g, kind)
    else:
        for copy in loads[2:]:
            copy.wait()
        for g in range(chunks):
            first_wait(g, 0)
            each(lambda b: score(g, b), qblocks)
            first_wait(g, 1)
            each(lambda b: mix(g, b), qblocks)
            project_all(g)
    for lane in range(len(first)):
        for g in range(chunks):
            for kind in range(2):
                first_copy(lane, g, kind).wait_send()


def per_device(queries, keys, values, residual, w_out, neighbours, band_start, band_blocks, band_count):
    tokens, width = queries.shape[1:]
    qblocks = band_count.shape[2]
    most = band_blocks.shape[3]
    cameras = lax.axis_size("cam")
    rigs = cameras // min(32, cameras)
    chunks = width // LANES
    head_dim = width // HEADS
    cfg = (cameras, rigs, chunks, qblocks, most, head_dim)
    relay = relays(cameras, rigs)
    lanes = 1 if relay else ROLES
    dma = pltpu.SemaphoreType.DMA
    anywhere = pl.BlockSpec(memory_space=pltpu.HBM)
    scalars = pl.BlockSpec(memory_space=pltpu.SMEM)
    block_len = tokens // qblocks
    blocks = (qblocks, block_len, width)
    heads = LANES // head_dim
    pair = 2 if chunks % 2 == 0 else 1
    bf16 = jnp.bfloat16
    regular = pltpu.SemaphoreType.REGULAR
    scratch = []
    for kind in range(2):
        for role in range(ROLES):
            for g in range(chunks):
                count = WIN if relay and role == ROLES - 1 else qblocks
                scratch += [pltpu.VMEM((count, block_len // n, LANES), bf16) for n in cuts(cfg, role, g, kind)]
    scratch += [pltpu.VMEM(blocks, bf16)] * 4 + [
        pltpu.VMEM((width, width), bf16),
        pltpu.VMEM((qblocks, heads * block_len, (1 + ROLES * most) * block_len), bf16),
        pltpu.VMEM((qblocks * block_len, pair * LANES), bf16),
        pltpu.VMEM(blocks, jnp.float32),
        dma((5,)),
        dma((lanes, chunks, 2)),
        dma((lanes, chunks, 2)),
    ]
    if relay:
        scratch += [pltpu.VMEM((qblocks, heads * block_len, LANES), jnp.float32), regular, regular, pltpu.SMEM((2, 1, ROLES), jnp.int32), pltpu.SMEM((2, 1, ROLES), jnp.int32), dma((2, 2)), dma((2, 2))]
        scratch += [dma((chunks, 2))] * 5 + [dma((chunks, 2, max(len(c) for c in CUTS)))]
        for kind in range(2):
            for g in range(chunks):
                for n in cuts(cfg, X_ROLE, g, kind):
                    scratch += [pltpu.VMEM((WIN, block_len // n, LANES), bf16)] * 2
    out = pl.pallas_call(
        functools.partial(kernel, cfg),
        out_shape=pltpu.VMEM(blocks, bf16),
        in_specs=[anywhere] * 5 + [scalars] * 4,
        out_specs=pl.BlockSpec(memory_space=pltpu.VMEM),
        scratch_shapes=scratch,
        compiler_params=pltpu.CompilerParams(
            collective_id=0, has_side_effects=True, vmem_limit_bytes=VMEM_LIMIT * 1024 * 1024
        ),
        name="band_attention",
    )(
        *(x[0].reshape(blocks) for x in (queries, keys, values, residual)),
        w_out, neighbours, band_start, jnp.swapaxes(band_blocks, 2, 3), band_count,
    )
    return out.reshape(tokens, width)[None]


VMEM_LIMIT = 62
CUTS = ((2, 2), (2, 4, 8, 8))
LAST = 6
GROUP = 3
TAIL = 6
TAIL_UNROLL = 1


def solution(mesh):
    rows = ("scene", "cam")
    return jax.shard_map(
        per_device,
        mesh=mesh,
        in_specs=(
            P(rows, None, None),
            P(rows, None, None),
            P(rows, None, None),
            P(rows, None, None),
            P(),
            P(rows, None),
            P(rows, None),
            P(rows, None, None, None),
            P(rows, None, None),
        ),
        out_specs=P(rows, None, None),
        check_vma=False,
    )
```

```python
import functools
import math

import jax
import jax.numpy as jnp
from jax import lax
from jax.experimental import pallas as pl
from jax.experimental.pallas import tpu as pltpu
from jax.sharding import PartitionSpec as P

HEADS = 16
LANES = 128
ROLES = 4
WIN = 3
X_ROLE = 1
HIDDEN = -1e30
MESH = pl.DeviceIdType.MESH


def relays(cameras, rigs):
    return rigs == 1 and cameras % 4 == 0


def cuts(cfg, role, g, kind):
    cameras, rigs, chunks = cfg[:3]
    if role != X_ROLE or not relays(cameras, rigs) or g < chunks - 1:
        return (1,)
    return CUTS[kind]


def kernel(cfg, q_hbm, k_hbm, v_hbm, r_hbm, w_hbm, near_hbm, start_hbm, block_hbm, count_hbm, out_ref, *scratch):
    cameras, rigs, chunks, qblocks, most, head_dim = cfg
    relay = relays(cameras, rigs)
    take = iter(scratch)
    part_a, part_x, part_b, part_z = range(ROLES)
    near = [
        [[[next(take) for _ in cuts(cfg, role, g, kind)] for g in range(chunks)] for role in range(ROLES)]
        for kind in range(2)
    ]
    q_ref, own_k, own_v, r_ref, w_ref, probs_ref, att_ref, acc_ref, own_sem = [next(take) for _ in range(9)]
    first_send, first_recv = next(take), next(take)
    near_ref, start_ref, block_ref, count_ref, table_sem = [next(take) for _ in range(5)]
    if relay:
        mixed_ref, near_sem, far_sem, told_near, told_start, tell_send, tell_recv = [next(take) for _ in range(7)]
        x_send, z_send, b_send, z_recv, b_recv, x_recv = [next(take) for _ in range(6)]
        staged = [
            [[[next(take) for _ in range(2)] for _ in cuts(cfg, part_x, g, kind)] for g in range(chunks)]
            for kind in range(2)
        ]
    own = (own_k, own_v)
    block_len = q_ref.shape[1]
    heads = LANES // head_dim
    pair = 2 if chunks % 2 == 0 else 1
    me = lax.axis_index("cam")

    def at(offset):
        return lax.rem(me + offset + 2 * cameras, cameras)

    if relay:
        column = lax.rem(me // 2, 2)
        core = lax.rem(me, 2)
        partner = me + 1 - 2 * core
        across = me + 2 - 4 * column
        z_to = at(4 - 8 * column)
        z_from = at(8 * column - 4)
        from_x = lax.rem(column + core, 2) == 0
        z_view = at(4 * column - 2)
        partner_x = partner + 2 - 4 * column
        partner_z = lax.rem(partner + 4 * column - 2 + cameras, cameras)
        b_view = jnp.where(from_x, partner_z, partner_x)
        views = (partner, across, b_view, z_view)
        first = ((part_a, partner),)
    else:
        views = (at(rigs), at(-rigs), at(2 * rigs), at(-2 * rigs))
        first = ((0, views[1]), (1, views[0]), (2, views[3]), (3, views[2]))

    loads = [
        pltpu.make_async_copy(src, dst, own_sem.at[n])
        for n, (src, dst) in enumerate(
            ((k_hbm, own_k), (v_hbm, own_v), (q_hbm, q_ref), (w_hbm, w_ref), (r_hbm, r_ref))
        )
    ]
    tables = [
        pltpu.make_async_copy(src, dst, table_sem.at[n])
        for n, (src, dst) in enumerate(
            ((near_hbm, near_ref), (start_hbm, start_ref), (block_hbm, block_ref), (count_hbm, count_ref))
        )
    ]
    for copy in tables + loads[:2]:
        copy.start()

    def signal(sem, peer):
        pl.semaphore_signal(sem, inc=1, device_id={"cam": peer}, device_id_type=MESH)

    barrier = pltpu.get_barrier_semaphore()
    if relay:
        signal(barrier, across - core)
        signal(barrier, z_from + 1 - core)
        signal(barrier, z_to + 1 - core)

        @pl.when(core == 1)
        def _():
            signal(barrier, partner)

        @pl.when(core == 0)
        def _():
            pl.semaphore_wait(barrier, 3)
            signal(near_sem, partner)

        @pl.when(core == 1)
        def _():
            pl.semaphore_wait(near_sem, 1)
    else:
        for view in views:
            signal(barrier, view)
        pl.semaphore_wait(barrier, len(views))

    def remote(src, dst, send, recv, target):
        return pltpu.make_async_remote_copy(
            src_ref=src, dst_ref=dst, send_sem=send, recv_sem=recv,
            device_id={"cam": target}, device_id_type=MESH,
        )

    def cols(g):
        return slice(g * LANES, (g + 1) * LANES)

    def first_copy(lane, g, kind):
        role, target = first[lane]
        return remote(
            own[kind].at[:, :, cols(g)], near[kind][role][g][0],
            first_send.at[lane, g, kind], first_recv.at[lane, g, kind], target,
        )

    def rows(g, kind, part):
        sizes = [block_len // n for n in cuts(cfg, part_x, g, kind)]
        return pl.ds(sum(sizes[:part]), sizes[part])

    def x_copy(g, kind, part):
        source = own if g else (k_hbm, v_hbm)
        return remote(
            source[kind].at[:, rows(g, kind, part), cols(g)], near[kind][part_x][g][part],
            x_send.at[g, kind], x_recv.at[g, kind, part], across,
        )

    def z_copy(g, kind, part):
        return remote(
            staged[kind][g][part][0], near[kind][part_z][g][0].at[:, rows(g, kind, part)],
            z_send.at[g, kind], z_recv.at[g, kind], z_to,
        )

    def far_copy(g, kind, part):
        return remote(
            staged[kind][g][part][1], near[kind][part_b][g][0].at[pl.ds(0, WIN), rows(g, kind, part)],
            b_send.at[g, kind], b_recv.at[g, kind], z_to + 1 - 2 * core,
        )

    def near_copy(g, kind, part):
        return remote(
            near[kind][part_x][g][part], near[kind][part_b][g][0].at[:, rows(g, kind, part)],
            b_send.at[g, kind], b_recv.at[g, kind], partner,
        )

    def whole(g, kind, role, send, recv):
        buffer = near[kind][role][g][0]
        return remote(buffer, buffer, send.at[g, kind], recv.at[g, kind], partner)

    def each(body, count=qblocks, unroll=1):
        def step(b, carry):
            body(b)
            return carry

        lax.fori_loop(0, count, step, 0, unroll=unroll)

    def listed(r, b, m):
        index = starts[r] + block_ref[0, slots[r], m, b]
        if m == 0:
            return index, None
        live = m < count_ref[0, slots[r], b]
        return jnp.where(live, index, 0), jnp.where(live, 0.0, HIDDEN)

    def score(g, b):
        q = q_ref[b, :, cols(g)] * jnp.asarray(1.0 / math.sqrt(head_dim), jnp.bfloat16)
        lane = lax.broadcasted_iota(jnp.int32, (block_len, LANES), 1) // head_dim
        q2 = jnp.concatenate([jnp.where(lane == h, q, jnp.zeros_like(q)) for h in range(heads)], axis=0)
        dims = (((1,), (1,)), ((), ()))

        def dot(keys):
            return lax.dot_general(q2, keys, dims, preferred_element_type=jnp.float32)

        scores = [dot(own_k[b, :, cols(g)])]
        for r in range(ROLES):
            found = [listed(r, b, m) for m in range(most)]
            got = dot(jnp.concatenate([part[index] for index, _ in found for part in near[0][r][g]], axis=0))
            for m, (_, bias) in enumerate(found):
                piece = got[:, m * block_len:(m + 1) * block_len]
                scores.append(piece if bias is None else piece + bias)
        scores = jnp.concatenate(scores, axis=1)
        top = jnp.max(scores, axis=1, keepdims=True)
        expo = jnp.exp(scores - top)
        total = jnp.sum(expo, axis=1, keepdims=True)
        probs_ref[b] = (expo * (1.0 / total)).astype(jnp.bfloat16)

    def weigh(g, b, roles):
        vals = []
        for r in roles:
            if r < 0:
                vals.append(own_v[b, :, cols(g)])
            else:
                vals += [part[listed(r, b, m)[0]] for m in range(most) for part in near[1][r][g]]
        low = 0 if roles[0] < 0 else (1 + roles[0] * most) * block_len
        high = (1 + (roles[-1] + 1) * most) * block_len
        return jnp.dot(probs_ref[b, :, low:high], jnp.concatenate(vals, axis=0), preferred_element_type=jnp.float32)

    def early(g, b):
        mixed_ref[b] = weigh(g, b, (-1, part_a, part_x))

    def late(g, b):
        finish(g, b, mixed_ref[b] + weigh(g, b, (part_b, part_z)))

    def mix(g, b):
        finish(g, b, weigh(g, b, tuple(range(-1, ROLES))))

    def finish(g, b, mixed):
        lane = lax.broadcasted_iota(jnp.int32, (block_len, LANES), 1) // head_dim
        result = mixed[:block_len]
        for h in range(1, heads):
            result = jnp.where(lane == h, mixed[h * block_len:(h + 1) * block_len], result)
        half = g % pair
        place = pl.ds(pl.multiple_of(b * block_len, block_len), block_len)
        att_ref[place, half * LANES:(half + 1) * LANES] = result.astype(jnp.bfloat16)

    def project(g, group, count):
        half = g % pair
        if half < pair - 1:
            return
        place = pl.ds(pl.multiple_of(group * count * block_len, block_len), count * block_len)
        rows = slice((g - half) * LANES, (g + 1) * LANES)
        added = jnp.dot(att_ref[place, :], w_ref[rows, :], preferred_element_type=jnp.float32)
        for n in range(count):
            b = group * count + n
            base = r_ref[b].astype(jnp.float32) if g == half else acc_ref[b]
            summed = base + added[n * block_len:(n + 1) * block_len]
            if g == chunks - 1:
                out_ref[b] = summed.astype(out_ref.dtype)
            else:
                acc_ref[b] = summed

    def project_all(g):
        count = GROUP if qblocks % GROUP == 0 else 1
        each(lambda group: project(g, group, count), qblocks // count)

    parts = [(g, kind, part) for g in range(chunks) for kind in range(2) for part in range(len(cuts(cfg, part_x, g, kind)))]
    if relay:
        for g, kind, part in parts:
            if g == 0:
                x_copy(g, kind, part).start()
    for copy in loads[:2]:
        copy.wait()
    if relay:
        for g, kind, part in parts:
            if g > 0:
                x_copy(g, kind, part).start()
    for copy in loads[2:]:
        copy.start()
    for lane in range(len(first)):
        for g in range(chunks):
            for kind in range(2):
                first_copy(lane, g, kind).start()
    for copy in tables:
        copy.wait()
    slots = []
    for view in views:
        slot = jnp.int32(0)
        for s in range(1, ROLES):
            slot = jnp.where(near_ref[0, s] == view, s, slot)
        slots.append(slot)
    starts = [start_ref[0, slot] for slot in slots]
    if relay:
        starts[part_z] = jnp.int32(0)
        starts[part_b] = jnp.where(from_x, 0, starts[part_b])

    def first_wait(g, kind):
        for lane in range(len(first)):
            first_copy(lane, g, kind).wait_recv()

    if relay:

        @pl.when(core == 1)
        def _():
            pl.semaphore_wait(barrier, 4)
            signal(far_sem, partner)

        @pl.when(core == 0)
        def _():
            pl.semaphore_wait(far_sem, 1)

        def tell(n, k):
            row, place = ((near_ref, told_near), (start_ref, told_start))[k]
            return remote(row, place.at[core], tell_send.at[n, k], tell_recv.at[core, k], z_from - core + n)

        def told(n, view):
            start = told_start[n, 0, 0]
            for s in range(1, ROLES):
                start = jnp.where(told_near[n, 0, s] == view, told_start[n, 0, s], start)
            return start

        for n in range(2):
            for k in range(2):
                tell(n, k).start()
        for n in range(2):
            for k in range(2):
                tell(n, k).wait_send()
        for n in range(2):
            for k in range(2):
                remote(
                    told_near.at[n], (told_near, told_start)[k].at[n], tell_send.at[n, k], tell_recv.at[n, k], partner
                ).wait_recv()
        start_z = told(core, across)
        start_b = told(1 - core, across)

        def relay_part(g, kind, part):
            x_copy(g, kind, part).wait_recv()
            source = near[kind][part_x][g][part]
            for n in range(WIN):
                staged[kind][g][part][0][n] = source[start_z + n]
            z_copy(g, kind, part).start()

            @pl.when(from_x)
            def _():
                near_copy(g, kind, part).start()

            @pl.when(jnp.logical_not(from_x))
            def _():
                for n in range(WIN):
                    staged[kind][g][part][1][n] = source[start_b + n]
                far_copy(g, kind, part).start()

        def arrive(g, kind, all_roles=True):
            if all_roles:
                first_wait(g, kind)

            @pl.when(from_x)
            def _():
                whole(g, kind, part_z, b_send, b_recv).wait_recv()

            @pl.when(jnp.logical_not(from_x))
            def _():
                whole(g, kind, part_b, b_send, b_recv).wait_recv()

            whole(g, kind, part_z, z_send, z_recv).wait_recv()

        def drain(g, kind):
            whole(g, kind, part_b, x_send, b_recv).wait_send()
            whole(g, kind, part_z, z_send, b_recv).wait_send()

            @pl.when(from_x)
            def _():
                whole(g, kind, part_b, b_send, b_recv).wait_send()

            @pl.when(jnp.logical_not(from_x))
            def _():
                whole(g, kind, part_z, b_send, b_recv).wait_send()

        def run(work, g, kind, low, high, unroll=2):
            if low == 0:
                arrive(g, kind)
            count = high - low
            each(lambda b: work(g, low + b), count, unroll if count % unroll == 0 else 1)
            if work is mix and high == qblocks:
                project_all(g)

        end = chunks - 1
        for g, kind, part in parts:
            relay_part(g, kind, part)
            if g == 1 and kind == 0 and part == 0:
                for copy in loads[2:]:
                    copy.wait()
            if g == 0:
                continue
            if g < end:
                run((score, mix)[kind], g - 1, kind, 0, qblocks)
                if g >= 2:
                    drain(g - 2, kind)
            elif kind == 0:
                n = len(cuts(cfg, part_x, g, kind))
                run(score, g - 1, 0, part * qblocks // n, (part + 1) * qblocks // n, 3)
            elif part in MIX_AFTER:
                n = MIX_AFTER.index(part)
                size = qblocks // len(MIX_AFTER)
                run(mix, g - 1, 1, n * size, (n + 1) * size, 3)
        run(score, end, 0, 0, qblocks)
        first_wait(end, 1)
        each(lambda b: early(end, b), qblocks, LAST)
        arrive(end, 1, False)
        count = TAIL if qblocks % TAIL == 0 else 1

        def close(group):
            for n in range(count):
                late(end, group * count + n)
            project(end, group, count)

        each(close, qblocks // count, TAIL_UNROLL)
        for g in range(max(0, end - 2), chunks):
            for kind in range(2):
                drain(g, kind)
    else:
        for copy in loads[2:]:
            copy.wait()
        for g in range(chunks):
            first_wait(g, 0)
            each(lambda b: score(g, b), qblocks)
            first_wait(g, 1)
            each(lambda b: mix(g, b), qblocks)
            project_all(g)
    for lane in range(len(first)):
        for g in range(chunks):
            for kind in range(2):
                first_copy(lane, g, kind).wait_send()


def per_device(queries, keys, values, residual, w_out, neighbours, band_start, band_blocks, band_count):
    tokens, width = queries.shape[1:]
    qblocks = band_count.shape[2]
    most = band_blocks.shape[3]
    cameras = lax.axis_size("cam")
    rigs = cameras // min(32, cameras)
    chunks = width // LANES
    head_dim = width // HEADS
    cfg = (cameras, rigs, chunks, qblocks, most, head_dim)
    relay = relays(cameras, rigs)
    lanes = 1 if relay else ROLES
    dma = pltpu.SemaphoreType.DMA
    anywhere = pl.BlockSpec(memory_space=pltpu.HBM)
    block_len = tokens // qblocks
    blocks = (qblocks, block_len, width)
    heads = LANES // head_dim
    pair = 2 if chunks % 2 == 0 else 1
    bf16 = jnp.bfloat16
    regular = pltpu.SemaphoreType.REGULAR
    scratch = []
    for kind in range(2):
        for role in range(ROLES):
            for g in range(chunks):
                count = WIN if relay and role == ROLES - 1 else qblocks
                scratch += [pltpu.VMEM((count, block_len // n, LANES), bf16) for n in cuts(cfg, role, g, kind)]
    scratch += [pltpu.VMEM(blocks, bf16)] * 4 + [
        pltpu.VMEM((width, width), bf16),
        pltpu.VMEM((qblocks, heads * block_len, (1 + ROLES * most) * block_len), bf16),
        pltpu.VMEM((qblocks * block_len, pair * LANES), bf16),
        pltpu.VMEM(blocks, jnp.float32),
        dma((5,)),
        dma((lanes, chunks, 2)),
        dma((lanes, chunks, 2)),
    ]
    tables = (neighbours, band_start, jnp.swapaxes(band_blocks, 2, 3), band_count)
    scratch += [pltpu.SMEM(table.shape, table.dtype) for table in tables] + [dma((4,))]
    if relay:
        scratch += [pltpu.VMEM((qblocks, heads * block_len, LANES), jnp.float32), regular, regular, pltpu.SMEM((2, 1, ROLES), jnp.int32), pltpu.SMEM((2, 1, ROLES), jnp.int32), dma((2, 2)), dma((2, 2))]
        scratch += [dma((chunks, 2))] * 5 + [dma((chunks, 2, max(len(c) for c in CUTS)))]
        for kind in range(2):
            for g in range(chunks):
                for n in cuts(cfg, X_ROLE, g, kind):
                    scratch += [pltpu.VMEM((WIN, block_len // n, LANES), bf16)] * 2
    out = pl.pallas_call(
        functools.partial(kernel, cfg),
        out_shape=pltpu.VMEM(blocks, bf16),
        in_specs=[anywhere] * 9,
        out_specs=pl.BlockSpec(memory_space=pltpu.VMEM),
        scratch_shapes=scratch,
        compiler_params=pltpu.CompilerParams(
            collective_id=0, has_side_effects=True, vmem_limit_bytes=VMEM_LIMIT * 1024 * 1024
        ),
        name="band_attention",
    )(
        *(x[0].reshape(blocks) for x in (queries, keys, values, residual)),
        w_out, *tables,
    )
    return out.reshape(tokens, width)[None]


VMEM_LIMIT = 62
CUTS = ((2, 2), (2, 4, 8, 8))
LAST = 6
GROUP = 3
TAIL = 6
MIX_AFTER = (1, 3)
TAIL_UNROLL = 1


def solution(mesh):
    rows = ("scene", "cam")
    return jax.shard_map(
        per_device,
        mesh=mesh,
        in_specs=(
            P(rows, None, None),
            P(rows, None, None),
            P(rows, None, None),
            P(rows, None, None),
            P(),
            P(rows, None),
            P(rows, None),
            P(rows, None, None, None),
            P(rows, None, None),
        ),
        out_specs=P(rows, None, None),
        check_vma=False,
    )
```

```python
import functools
import math

import jax
import jax.numpy as jnp
from jax import lax
from jax.experimental import pallas as pl
from jax.experimental.pallas import tpu as pltpu
from jax.sharding import PartitionSpec as P

HEADS = 16
LANES = 128
ROLES = 4
WIN = 3
X_ROLE = 1
HIDDEN = -1e30
MESH = pl.DeviceIdType.MESH


def relays(cameras, rigs):
    return rigs == 1 and cameras % 4 == 0


def cuts(cfg, role, g, kind):
    cameras, rigs, chunks = cfg[:3]
    if role != X_ROLE or not relays(cameras, rigs) or g < chunks - 1:
        return (1,)
    return CUTS[kind]


def kernel(cfg, q_hbm, k_hbm, v_hbm, r_hbm, w_hbm, near_hbm, start_hbm, block_hbm, count_hbm, out_ref, *scratch):
    cameras, rigs, chunks, qblocks, most, head_dim = cfg
    relay = relays(cameras, rigs)
    take = iter(scratch)
    part_a, part_x, part_b, part_z = range(ROLES)
    near = [
        [[[next(take) for _ in cuts(cfg, role, g, kind)] for g in range(chunks)] for role in range(ROLES)]
        for kind in range(2)
    ]
    q_ref, own_k, own_v, r_ref, w_ref, probs_ref, att_ref, acc_ref, own_sem = [next(take) for _ in range(9)]
    first_send, first_recv = next(take), next(take)
    near_ref, start_ref, block_ref, count_ref, table_sem, head_ref = [next(take) for _ in range(6)]
    if relay:
        mixed_ref, near_sem, far_sem, told_near, told_start, tell_send, tell_recv = [next(take) for _ in range(7)]
        x_send, z_send, b_send, z_recv, b_recv, x_recv = [next(take) for _ in range(6)]
        staged = [
            [[[next(take) for _ in range(2)] for _ in cuts(cfg, part_x, g, kind)] for g in range(chunks)]
            for kind in range(2)
        ]
    own = (own_k, own_v)
    block_len = q_ref.shape[1]
    heads = LANES // head_dim
    pair = 2 if chunks % 2 == 0 else 1
    me = lax.axis_index("cam")

    def at(offset):
        return lax.rem(me + offset + 2 * cameras, cameras)

    if relay:
        column = lax.rem(me // 2, 2)
        core = lax.rem(me, 2)
        partner = me + 1 - 2 * core
        across = me + 2 - 4 * column
        z_to = at(4 - 8 * column)
        z_from = at(8 * column - 4)
        from_x = lax.rem(column + core, 2) == 0
        z_view = at(4 * column - 2)
        partner_x = partner + 2 - 4 * column
        partner_z = lax.rem(partner + 4 * column - 2 + cameras, cameras)
        b_view = jnp.where(from_x, partner_z, partner_x)
        views = (partner, across, b_view, z_view)
        first = ((part_a, partner),)
    else:
        views = (at(rigs), at(-rigs), at(2 * rigs), at(-2 * rigs))
        first = ((0, views[1]), (1, views[0]), (2, views[3]), (3, views[2]))

    loads = [
        pltpu.make_async_copy(src, dst, own_sem.at[n])
        for n, (src, dst) in enumerate(
            ((k_hbm, own_k), (v_hbm, own_v), (q_hbm, q_ref), (w_hbm, w_ref), (r_hbm, r_ref))
        )
    ]
    tables = [
        pltpu.make_async_copy(src, dst, table_sem.at[n])
        for n, (src, dst) in enumerate(
            ((near_hbm, near_ref), (start_hbm, start_ref), (block_hbm, block_ref), (count_hbm, count_ref))
        )
    ]
    head = pltpu.make_async_copy(k_hbm.at[:, :, :LANES], head_ref, table_sem.at[4])
    for copy in [head] + tables + loads[:2]:
        copy.start()

    def signal(sem, peer):
        pl.semaphore_signal(sem, inc=1, device_id={"cam": peer}, device_id_type=MESH)

    barrier = pltpu.get_barrier_semaphore()
    if relay:
        signal(barrier, across - core)
        signal(barrier, z_from + 1 - core)
        signal(barrier, z_to + 1 - core)

        @pl.when(core == 1)
        def _():
            signal(barrier, partner)

        @pl.when(core == 0)
        def _():
            pl.semaphore_wait(barrier, 3)
            signal(near_sem, partner)

        @pl.when(core == 1)
        def _():
            pl.semaphore_wait(near_sem, 1)
    else:
        for view in views:
            signal(barrier, view)
        pl.semaphore_wait(barrier, len(views))

    def remote(src, dst, send, recv, target):
        return pltpu.make_async_remote_copy(
            src_ref=src, dst_ref=dst, send_sem=send, recv_sem=recv,
            device_id={"cam": target}, device_id_type=MESH,
        )

    def cols(g):
        return slice(g * LANES, (g + 1) * LANES)

    def first_copy(lane, g, kind):
        role, target = first[lane]
        return remote(
            own[kind].at[:, :, cols(g)], near[kind][role][g][0],
            first_send.at[lane, g, kind], first_recv.at[lane, g, kind], target,
        )

    def rows(g, kind, part):
        sizes = [block_len // n for n in cuts(cfg, part_x, g, kind)]
        return pl.ds(sum(sizes[:part]), sizes[part])

    def x_copy(g, kind, part):
        if g == kind == 0:
            source = head_ref.at[:, rows(g, kind, part)]
        else:
            source = (own if g else (k_hbm, v_hbm))[kind].at[:, rows(g, kind, part), cols(g)]
        return remote(
            source, near[kind][part_x][g][part],
            x_send.at[g, kind], x_recv.at[g, kind, part], across,
        )

    def z_copy(g, kind, part):
        return remote(
            staged[kind][g][part][0], near[kind][part_z][g][0].at[:, rows(g, kind, part)],
            z_send.at[g, kind], z_recv.at[g, kind], z_to,
        )

    def far_copy(g, kind, part):
        return remote(
            staged[kind][g][part][1], near[kind][part_b][g][0].at[pl.ds(0, WIN), rows(g, kind, part)],
            b_send.at[g, kind], b_recv.at[g, kind], z_to + 1 - 2 * core,
        )

    def near_copy(g, kind, part):
        return remote(
            near[kind][part_x][g][part], near[kind][part_b][g][0].at[:, rows(g, kind, part)],
            b_send.at[g, kind], b_recv.at[g, kind], partner,
        )

    def whole(g, kind, role, send, recv):
        buffer = near[kind][role][g][0]
        return remote(buffer, buffer, send.at[g, kind], recv.at[g, kind], partner)

    def each(body, count=qblocks, unroll=1):
        def step(b, carry):
            body(b)
            return carry

        lax.fori_loop(0, count, step, 0, unroll=unroll)

    def listed(r, b, m):
        index = starts[r] + block_ref[0, slots[r], m, b]
        if m == 0:
            return index, None
        live = m < count_ref[0, slots[r], b]
        return jnp.where(live, index, 0), jnp.where(live, 0.0, HIDDEN)

    def score(g, b):
        q = q_ref[b, :, cols(g)] * jnp.asarray(1.0 / math.sqrt(head_dim), jnp.bfloat16)
        lane = lax.broadcasted_iota(jnp.int32, (block_len, LANES), 1) // head_dim
        q2 = jnp.concatenate([jnp.where(lane == h, q, jnp.zeros_like(q)) for h in range(heads)], axis=0)
        dims = (((1,), (1,)), ((), ()))

        def dot(keys):
            return lax.dot_general(q2, keys, dims, preferred_element_type=jnp.float32)

        scores = [dot(own_k[b, :, cols(g)])]
        for r in range(ROLES):
            found = [listed(r, b, m) for m in range(most)]
            got = dot(jnp.concatenate([part[index] for index, _ in found for part in near[0][r][g]], axis=0))
            for m, (_, bias) in enumerate(found):
                piece = got[:, m * block_len:(m + 1) * block_len]
                scores.append(piece if bias is None else piece + bias)
        scores = jnp.concatenate(scores, axis=1)
        top = jnp.max(scores, axis=1, keepdims=True)
        expo = jnp.exp(scores - top)
        total = jnp.sum(expo, axis=1, keepdims=True)
        probs_ref[b] = (expo * (1.0 / total)).astype(jnp.bfloat16)

    def weigh(g, b, roles):
        vals = []
        for r in roles:
            if r < 0:
                vals.append(own_v[b, :, cols(g)])
            else:
                vals += [part[listed(r, b, m)[0]] for m in range(most) for part in near[1][r][g]]
        low = 0 if roles[0] < 0 else (1 + roles[0] * most) * block_len
        high = (1 + (roles[-1] + 1) * most) * block_len
        return jnp.dot(probs_ref[b, :, low:high], jnp.concatenate(vals, axis=0), preferred_element_type=jnp.float32)

    def early(g, b):
        mixed_ref[b] = weigh(g, b, (-1, part_a, part_x))

    def late(g, b):
        finish(g, b, mixed_ref[b] + weigh(g, b, (part_b, part_z)))

    def mix(g, b):
        finish(g, b, weigh(g, b, tuple(range(-1, ROLES))))

    def finish(g, b, mixed):
        lane = lax.broadcasted_iota(jnp.int32, (block_len, LANES), 1) // head_dim
        result = mixed[:block_len]
        for h in range(1, heads):
            result = jnp.where(lane == h, mixed[h * block_len:(h + 1) * block_len], result)
        half = g % pair
        place = pl.ds(pl.multiple_of(b * block_len, block_len), block_len)
        att_ref[place, half * LANES:(half + 1) * LANES] = result.astype(jnp.bfloat16)

    def project(g, group, count):
        half = g % pair
        if half < pair - 1:
            return
        place = pl.ds(pl.multiple_of(group * count * block_len, block_len), count * block_len)
        rows = slice((g - half) * LANES, (g + 1) * LANES)
        added = jnp.dot(att_ref[place, :], w_ref[rows, :], preferred_element_type=jnp.float32)
        for n in range(count):
            b = group * count + n
            base = r_ref[b].astype(jnp.float32) if g == half else acc_ref[b]
            summed = base + added[n * block_len:(n + 1) * block_len]
            if g == chunks - 1:
                out_ref[b] = summed.astype(out_ref.dtype)
            else:
                acc_ref[b] = summed

    def project_all(g):
        count = GROUP if qblocks % GROUP == 0 else 1
        each(lambda group: project(g, group, count), qblocks // count)

    parts = [(g, kind, part) for g in range(chunks) for kind in range(2) for part in range(len(cuts(cfg, part_x, g, kind)))]
    head.wait()
    if relay:
        for g, kind, part in parts:
            if g == 0:
                x_copy(g, kind, part).start()
    for copy in loads[:2]:
        copy.wait()
    if relay:
        for g, kind, part in parts:
            if g > 0:
                x_copy(g, kind, part).start()
    for copy in loads[2:]:
        copy.start()
    for lane in range(len(first)):
        for g in range(chunks):
            for kind in range(2):
                first_copy(lane, g, kind).start()
    for copy in tables:
        copy.wait()
    slots = []
    for view in views:
        slot = jnp.int32(0)
        for s in range(1, ROLES):
            slot = jnp.where(near_ref[0, s] == view, s, slot)
        slots.append(slot)
    starts = [start_ref[0, slot] for slot in slots]
    if relay:
        starts[part_z] = jnp.int32(0)
        starts[part_b] = jnp.where(from_x, 0, starts[part_b])

    def first_wait(g, kind):
        for lane in range(len(first)):
            first_copy(lane, g, kind).wait_recv()

    if relay:

        @pl.when(core == 1)
        def _():
            pl.semaphore_wait(barrier, 4)
            signal(far_sem, partner)

        @pl.when(core == 0)
        def _():
            pl.semaphore_wait(far_sem, 1)

        def tell(n, k):
            row, place = ((near_ref, told_near), (start_ref, told_start))[k]
            return remote(row, place.at[core], tell_send.at[n, k], tell_recv.at[core, k], z_from - core + n)

        def told(n, view):
            start = told_start[n, 0, 0]
            for s in range(1, ROLES):
                start = jnp.where(told_near[n, 0, s] == view, told_start[n, 0, s], start)
            return start

        for n in range(2):
            for k in range(2):
                tell(n, k).start()
        for n in range(2):
            for k in range(2):
                tell(n, k).wait_send()
        for n in range(2):
            for k in range(2):
                remote(
                    told_near.at[n], (told_near, told_start)[k].at[n], tell_send.at[n, k], tell_recv.at[n, k], partner
                ).wait_recv()
        start_z = told(core, across)
        start_b = told(1 - core, across)

        def relay_part(g, kind, part):
            x_copy(g, kind, part).wait_recv()
            source = near[kind][part_x][g][part]
            for n in range(WIN):
                staged[kind][g][part][0][n] = source[start_z + n]
            z_copy(g, kind, part).start()

            @pl.when(from_x)
            def _():
                near_copy(g, kind, part).start()

            @pl.when(jnp.logical_not(from_x))
            def _():
                for n in range(WIN):
                    staged[kind][g][part][1][n] = source[start_b + n]
                far_copy(g, kind, part).start()

        def arrive(g, kind, all_roles=True):
            if all_roles:
                first_wait(g, kind)

            @pl.when(from_x)
            def _():
                whole(g, kind, part_z, b_send, b_recv).wait_recv()

            @pl.when(jnp.logical_not(from_x))
            def _():
                whole(g, kind, part_b, b_send, b_recv).wait_recv()

            whole(g, kind, part_z, z_send, z_recv).wait_recv()

        def drain(g, kind):
            whole(g, kind, part_b, x_send, b_recv).wait_send()
            whole(g, kind, part_z, z_send, b_recv).wait_send()

            @pl.when(from_x)
            def _():
                whole(g, kind, part_b, b_send, b_recv).wait_send()

            @pl.when(jnp.logical_not(from_x))
            def _():
                whole(g, kind, part_z, b_send, b_recv).wait_send()

        def run(work, g, kind, low, high, unroll=2):
            if low == 0:
                arrive(g, kind)
            count = high - low
            each(lambda b: work(g, low + b), count, unroll if count % unroll == 0 else 1)
            if work is mix and high == qblocks:
                project_all(g)

        end = chunks - 1
        for g, kind, part in parts:
            relay_part(g, kind, part)
            if g == 1 and kind == 0 and part == 0:
                for copy in loads[2:]:
                    copy.wait()
            if g == 0:
                continue
            if g < end:
                run((score, mix)[kind], g - 1, kind, 0, qblocks)
                if g >= 2:
                    drain(g - 2, kind)
            elif kind == 0:
                n = len(cuts(cfg, part_x, g, kind))
                run(score, g - 1, 0, part * qblocks // n, (part + 1) * qblocks // n, 3)
            elif part in MIX_AFTER:
                n = MIX_AFTER.index(part)
                size = qblocks // len(MIX_AFTER)
                run(mix, g - 1, 1, n * size, (n + 1) * size, 3)
        run(score, end, 0, 0, qblocks)
        first_wait(end, 1)
        each(lambda b: early(end, b), qblocks, LAST)
        arrive(end, 1, False)
        count = TAIL if qblocks % TAIL == 0 else 1

        def close(group):
            for n in range(count):
                late(end, group * count + n)
            project(end, group, count)

        each(close, qblocks // count, TAIL_UNROLL)
        for g in range(max(0, end - 2), chunks):
            for kind in range(2):
                drain(g, kind)
    else:
        for copy in loads[2:]:
            copy.wait()
        for g in range(chunks):
            first_wait(g, 0)
            each(lambda b: score(g, b), qblocks)
            first_wait(g, 1)
            each(lambda b: mix(g, b), qblocks)
            project_all(g)
    for lane in range(len(first)):
        for g in range(chunks):
            for kind in range(2):
                first_copy(lane, g, kind).wait_send()


def per_device(queries, keys, values, residual, w_out, neighbours, band_start, band_blocks, band_count):
    tokens, width = queries.shape[1:]
    qblocks = band_count.shape[2]
    most = band_blocks.shape[3]
    cameras = lax.axis_size("cam")
    rigs = cameras // min(32, cameras)
    chunks = width // LANES
    head_dim = width // HEADS
    cfg = (cameras, rigs, chunks, qblocks, most, head_dim)
    relay = relays(cameras, rigs)
    lanes = 1 if relay else ROLES
    dma = pltpu.SemaphoreType.DMA
    anywhere = pl.BlockSpec(memory_space=pltpu.HBM)
    block_len = tokens // qblocks
    blocks = (qblocks, block_len, width)
    heads = LANES // head_dim
    pair = 2 if chunks % 2 == 0 else 1
    bf16 = jnp.bfloat16
    regular = pltpu.SemaphoreType.REGULAR
    scratch = []
    for kind in range(2):
        for role in range(ROLES):
            for g in range(chunks):
                count = WIN if relay and role == ROLES - 1 else qblocks
                scratch += [pltpu.VMEM((count, block_len // n, LANES), bf16) for n in cuts(cfg, role, g, kind)]
    scratch += [pltpu.VMEM(blocks, bf16)] * 4 + [
        pltpu.VMEM((width, width), bf16),
        pltpu.VMEM((qblocks, heads * block_len, (1 + ROLES * most) * block_len), bf16),
        pltpu.VMEM((qblocks * block_len, pair * LANES), bf16),
        pltpu.VMEM(blocks, jnp.float32),
        dma((5,)),
        dma((lanes, chunks, 2)),
        dma((lanes, chunks, 2)),
    ]
    tables = (neighbours, band_start, jnp.swapaxes(band_blocks, 2, 3), band_count)
    scratch += [pltpu.SMEM(table.shape, table.dtype) for table in tables] + [dma((5,)), pltpu.VMEM((qblocks, block_len, LANES), bf16)]
    if relay:
        scratch += [pltpu.VMEM((qblocks, heads * block_len, LANES), jnp.float32), regular, regular, pltpu.SMEM((2, 1, ROLES), jnp.int32), pltpu.SMEM((2, 1, ROLES), jnp.int32), dma((2, 2)), dma((2, 2))]
        scratch += [dma((chunks, 2))] * 5 + [dma((chunks, 2, max(len(c) for c in CUTS)))]
        for kind in range(2):
            for g in range(chunks):
                for n in cuts(cfg, X_ROLE, g, kind):
                    scratch += [pltpu.VMEM((WIN, block_len // n, LANES), bf16)] * 2
    out = pl.pallas_call(
        functools.partial(kernel, cfg),
        out_shape=pltpu.VMEM(blocks, bf16),
        in_specs=[anywhere] * 9,
        out_specs=pl.BlockSpec(memory_space=pltpu.VMEM),
        scratch_shapes=scratch,
        compiler_params=pltpu.CompilerParams(
            collective_id=0, has_side_effects=True, vmem_limit_bytes=VMEM_LIMIT * 1024 * 1024
        ),
        name="band_attention",
    )(
        *(x[0].reshape(blocks) for x in (queries, keys, values, residual)),
        w_out, *tables,
    )
    return out.reshape(tokens, width)[None]


VMEM_LIMIT = 62
CUTS = ((2, 2), (2, 4, 8, 8))
LAST = 6
GROUP = 3
TAIL = 6
MIX_AFTER = (1, 3)
TAIL_UNROLL = 1


def solution(mesh):
    rows = ("scene", "cam")
    return jax.shard_map(
        per_device,
        mesh=mesh,
        in_specs=(
            P(rows, None, None),
            P(rows, None, None),
            P(rows, None, None),
            P(rows, None, None),
            P(),
            P(rows, None),
            P(rows, None),
            P(rows, None, None, None),
            P(rows, None, None),
        ),
        out_specs=P(rows, None, None),
        check_vma=False,
    )
```
